32 devices in a mesh: dp: 8 (over y, x, core), mp: 4 (over z).
Axes of the slice: x: 2, y: 2, z: 4, core: 2. Of those that a mesh axis runs over, the one named last changes fastest.
Arguments:
- activations: bfloat16 [8192, 4096], P(('dp', 'mp')), may hold values from -17 to 17
- output_grads: bfloat16 [8192, 14336], P('dp', 'mp'), may hold values from -0.046875 to 0.046875
- q_start: float32 [14336, 64], P('mp'), may hold values from -6 to 6
Outputs:
- new_error: bfloat16 [32768, 14336], P('dp', 'mp')
- q_factor: float32 [14336, 64], P('mp')
The draws below stay inside these ranges and needn't reach their ends.
All inputs are finite; a program needn't handle non-finite values.
Results may differ from the reference program's by a relative error of at most 0.01.
Values may be sent and summed in bfloat16 or wider, within the bound.
A program may use at most 192 MiB of HBM per device.

```python
import jax
import jax.numpy as jnp
from jax import lax

D = 4096
FF = 14336
R = 64
TOK_REP = 1024
TOKENS = 8192
N_DP = 8


def draw_activations(key, part):
    key_base = jax.random.fold_in(key, 11)
    key_cols = jax.random.fold_in(key, 12)
    column = jnp.arange(D, dtype=jnp.float32) / D
    ramp = jnp.exp(jnp.log(3.0) * (column - 0.5))
    rough = jnp.exp(jax.random.uniform(key_cols, (D,), jnp.float32, -1.15, 1.15))
    scales = ramp * rough / 1.3
    base = jax.random.normal(key_base, (TOKENS, D), jnp.float32)
    base = jnp.clip(base, -4.0, 4.0)
    return (base * scales[None, :]).astype(jnp.bfloat16)


def shard_levels(rng, dims, split, least, largest):
    factor_of = 1.0
    for position, shards_of in split:
        draws = jax.random.uniform(jax.random.fold_in(jax.random.fold_in(rng, 6), position), (shards_of,), jnp.float32, least / len(split), largest / len(split))
        factor_of = factor_of * jnp.repeat(jnp.exp(draws), dims[position] // shards_of).reshape((-1,) + (1,) * (len(dims) - 1 - position))
    return factor_of


def normal_values(rng, shape, width, most, pieces=(), kind=jnp.bfloat16):
    array = width * jax.random.normal(rng, shape, jnp.float32)
    if pieces:
        array = array * shard_levels(rng, shape, pieces, -0.22, 0.18)
    return jnp.clip(array, -most, most).astype(kind)


def setup_inputs(seed: int = 0) -> dict:
    seeds = jax.random.split(jax.random.key(seed), 4)
    activations = draw_activations(jax.random.fold_in(seeds[3], 71), 0)
    output_grads = normal_values(seeds[1], (TOKENS, FF), (16 * TOK_REP) ** -0.5, 0.046875, ((0, 8), (1, 4)))
    q_start = normal_values(seeds[2], (FF, R), 1.0, 6.0, ((0, 4),), jnp.float32)
    return {"activations": activations, "output_grads": output_grads, "q_start": q_start}


def reference(activations, output_grads, q_start):
    highest = lax.Precision.HIGHEST
    inputs_rep = activations.reshape(N_DP, TOK_REP, D)
    grads_rep = output_grads.reshape(N_DP, TOK_REP, FF)

    def left_step(carry, pair):
        inputs, grads = pair
        projected = jnp.dot(grads.astype(jnp.float32), q_start, precision=highest)
        return (carry + jnp.dot(inputs.astype(jnp.float32).T, projected, precision=highest), None)
    p_summed, unused = lax.scan(left_step, jnp.zeros((D, R), jnp.float32), (inputs_rep, grads_rep))
    p_mean = p_summed / N_DP
    gram_matrix = jnp.dot(p_mean.T, p_mean, precision=highest)
    lower_tri = jnp.linalg.cholesky(gram_matrix)
    p_ortho = lax.linalg.triangular_solve(lower_tri, p_mean, left_side=False, lower=True, transpose_a=True)

    def right_step(carry, pair):
        inputs, grads = pair
        gradient = jnp.dot(inputs.T.astype(jnp.float32), grads.astype(jnp.float32), preferred_element_type=jnp.float32)
        return (carry + jnp.dot(gradient.T, p_ortho, precision=highest), None)
    q_summed, unused_two = lax.scan(right_step, jnp.zeros((FF, R), jnp.float32), (inputs_rep, grads_rep))
    q_factor = q_summed / N_DP
    decompressed = jnp.dot(p_ortho, q_factor.T, precision=highest)

    def error_one(pair):
        inputs, grads = pair
        gradient = jnp.dot(inputs.T.astype(jnp.float32), grads.astype(jnp.float32), preferred_element_type=jnp.float32)
        return (gradient - decompressed).astype(jnp.bfloat16)
    errors = lax.map(error_one, (inputs_rep, grads_rep))
    return (errors.reshape(N_DP * D, FF), q_factor)
```

```python
import functools

import jax
import jax.numpy as jnp
from jax import lax
from jax.experimental import pallas as pl
from jax.experimental.pallas import tpu as pltpu
from jax.sharding import PartitionSpec as P

ROWS = (((0,), (0,)), ((), ()))
COLS = (((1,), (1,)), ((), ()))
MESH = pl.DeviceIdType.MESH
F32 = jnp.float32
BF16 = jnp.bfloat16
CHUNKS = 16
EARLY = 11


def split_parts(values):
    upper = values.astype(BF16)
    lower = (values - upper.astype(F32)).astype(BF16)
    return (upper, lower)


def inverse_factor(gram):
    rank = gram.shape[0]
    row = lax.broadcasted_iota(jnp.int32, (rank, rank), 0)
    col = lax.broadcasted_iota(jnp.int32, (rank, rank), 1)
    left = gram
    right = jnp.where(row == col, 1.0, 0.0).astype(F32)
    down = lax.broadcasted_iota(jnp.int32, (rank, 1), 0)
    pivots = jnp.ones((rank, 1), F32)
    for k in range(rank):
        pivot = left[k : k + 1, k : k + 1]
        pivots = jnp.where(down == k, pivot, pivots)
        factor = jnp.where(down > k, left[:, k : k + 1] / pivot, 0.0)
        left_row = left[k : k + 1, :]
        right_row = right[k : k + 1, :]
        left = left - factor * left_row
        right = right - factor * right_row
    return right / jnp.sqrt(pivots)


class Exchange:
    def __init__(self, axis, count, me, source, target, send_sem, recv_sem):
        self.copies = []
        for shift in range(1, count):
            peer = lax.rem(me + shift, count)
            self.copies.append(
                pltpu.make_async_remote_copy(
                    src_ref=source(peer),
                    dst_ref=target,
                    send_sem=send_sem.at[shift],
                    recv_sem=recv_sem.at[shift],
                    device_id={axis: peer},
                    device_id_type=MESH,
                )
            )

    def start(self):
        for copy in self.copies:
            copy.start()

    def wait(self):
        for copy in self.copies:
            copy.wait()


def step_kernel(
    dims,
    x_hbm,
    y_hbm,
    q_ref,
    e_ref,
    q_out,
    xg,
    yv,
    xt,
    zpart,
    zrecv,
    part,
    recv,
    full,
    pmat,
    psum,
    pzr,
    pz,
    wall,
    local_sem,
    zs_sem,
    zr_sem,
    ps_sem,
    pr_sem,
    pzs_sem,
    pzr_sem,
    ags_sem,
    agr_sem,
    pgs_sem,
    pgr_sem,
    ws_sem,
    wr_sem,
    us_sem,
    ur_sem,
    uas_sem,
    uar_sem,
    right_send,
    right_recv,
    left_send,
    left_recv,
):
    replicas, shards = dims
    me = lax.axis_index("mp")
    rep = lax.axis_index("dp")
    tokens, depth = x_hbm.shape
    gathered, width = y_hbm.shape
    rank = q_ref.shape[1]
    lines = rank // replicas
    span = depth // shards
    chunk = depth // CHUNKS
    highest = lax.Precision.HIGHEST
    mine = pl.ds(pl.multiple_of(me * tokens, tokens), tokens)

    x_copy = pltpu.make_async_copy(x_hbm, xg.at[mine, :], local_sem.at[0])
    y_copy = pltpu.make_async_copy(y_hbm, yv.at[pl.ds(0, gathered), :], local_sem.at[1])
    x_copy.start()
    y_copy.start()

    barrier = pltpu.get_barrier_semaphore()
    for shift in range(1, shards):
        peer = lax.rem(me + shift, shards)
        pl.semaphore_signal(barrier, inc=1, device_id={"mp": peer}, device_id_type=MESH)
    for shift in range(1, replicas):
        peer = lax.rem(rep + shift, replicas)
        pl.semaphore_signal(barrier, inc=1, device_id={"dp": peer}, device_id_type=MESH)
    pl.semaphore_wait(barrier, shards + replicas - 2)

    def hop(owner, c, send_sem, recv_sem, target):
        rows = pl.ds(pl.multiple_of(owner * tokens, tokens), tokens)
        cols = pl.ds(pl.multiple_of(c * chunk, chunk), chunk)
        block = xg.at[rows, cols]
        return pltpu.make_async_remote_copy(
            src_ref=block,
            dst_ref=block,
            send_sem=send_sem,
            recv_sem=recv_sem,
            device_id={"mp": target},
            device_id_type=MESH,
        )

    def relay(step):
        for h in range(shards):
            c = step - h
            inside = jnp.logical_and(c >= 0, c < CHUNKS)
            for ahead, sends, recvs in ((True, right_send, right_recv), (False, left_send, left_recv)):
                owner = me - h if ahead else me + h
                exists = owner >= 0 if ahead else owner < shards
                onward = me < shards - 1 if ahead else me > 0
                target = me + 1 if ahead else me - 1
                source = me - 1 if ahead else me + 1
                if h >= 1:

                    @pl.when(jnp.logical_and(inside, exists))
                    def _():
                        hop(owner, c, sends.at[h - 1, c], recvs.at[h - 1, c], source).wait_recv()

                if h < shards - 1:

                    @pl.when(jnp.logical_and(inside, jnp.logical_and(exists, onward)))
                    def _():
                        hop(owner, c, sends.at[h, c], recvs.at[h, c], target).start()

    x_copy.wait()
    relay(0)

    q_cat = jnp.concatenate(split_parts(q_ref[...]), axis=1)
    zero_rows = xg.shape[0] - gathered - 3 * rank
    xg[pl.ds(gathered + 3 * rank, zero_rows), :] = jnp.zeros((zero_rows, depth), BF16)
    yv[pl.ds(gathered + 3 * rank, zero_rows), :] = jnp.zeros((zero_rows, width), BF16)
    y_copy.wait()
    both = jnp.dot(yv[pl.ds(0, gathered), :], q_cat, preferred_element_type=F32)
    both = both.T
    projected = both[:rank] + both[rank:]
    for j in range(shards):
        zpart[j] = projected[:, j * tokens : (j + 1) * tokens]
    z_move = Exchange("mp", shards, me, lambda peer: zpart.at[peer], zrecv.at[me], zs_sem, zr_sem)
    z_move.start()
    relay(1)
    z_move.wait()
    total = zpart[me]
    for shift in range(1, shards):
        total = total + zrecv[lax.rem(me + shift, shards)]

    z_cat = jnp.concatenate(split_parts(total), axis=0)
    both = jnp.dot(z_cat, xg[mine, :], preferred_element_type=F32)
    left = both[:rank] + both[rank:]
    for i in range(replicas):
        part[i] = left[i * lines : (i + 1) * lines, :]
    p_move = Exchange("dp", replicas, rep, lambda peer: part.at[peer], recv.at[rep], ps_sem, pr_sem)
    p_move.start()
    relay(2)
    p_move.wait()
    total = part[rep]
    for shift in range(1, replicas):
        total = total + recv[lax.rem(rep + shift, replicas)]
    for j in range(shards):
        psum[j] = total[:, j * span : (j + 1) * span]
    pz_move = Exchange("mp", shards, me, lambda peer: psum.at[peer], pzr.at[me], pzs_sem, pzr_sem)
    pz_move.start()
    relay(3)
    pz_move.wait()
    total = psum[me]
    for shift in range(1, shards):
        total = total + pzr[lax.rem(me + shift, shards)]
    pz[me] = total / replicas
    ag_move = Exchange("mp", shards, me, lambda peer: pz.at[me], pz.at[me], ags_sem, agr_sem)
    ag_move.start()
    relay(4)
    ag_move.wait()
    for j in range(shards):
        full[rep, :, pl.ds(j * span, span)] = pz[j]
    pg_move = Exchange("dp", replicas, rep, lambda peer: full.at[rep], full.at[rep], pgs_sem, pgr_sem)
    pg_move.start()
    relay(5)
    pg_move.wait()
    for i in range(replicas):
        pmat[pl.ds(i * lines, lines), :] = full[i]
    relay(6)

    p_mean = pmat[...]
    gram = lax.dot_general(p_mean, p_mean, COLS, precision=highest, preferred_element_type=F32)
    inverse = inverse_factor(gram)
    ortho = jnp.dot(inverse, pmat[...], precision=highest, preferred_element_type=F32)
    upper, lower = split_parts(-ortho)
    xg[pl.ds(gathered, rank), :] = upper
    xg[pl.ds(gathered + rank, rank), :] = upper
    xg[pl.ds(gathered + 2 * rank, rank), :] = lower
    relay(7)

    both = lax.dot_general(
        xg[pl.ds(gathered + rank, 2 * rank), :], xg[mine, :], COLS, preferred_element_type=F32
    )
    wall[me] = -(both[:rank] + both[rank:])
    w_move = Exchange("mp", shards, me, lambda peer: wall.at[me], wall.at[me], ws_sem, wr_sem)
    w_move.start()
    relay(8)
    w_move.wait()
    seen = jnp.concatenate([wall[j] for j in range(shards)], axis=1)
    w_cat = jnp.concatenate(split_parts(seen), axis=0)
    both = jnp.dot(w_cat, yv[pl.ds(0, gathered), :], preferred_element_type=F32)
    right = both[:rank] + both[rank:]
    used = pl.ds(0, width)
    for i in range(replicas):
        part[i, :, used] = right[i * lines : (i + 1) * lines, :]
    u_move = Exchange(
        "dp", replicas, rep, lambda peer: part.at[peer, :, used], recv.at[rep, :, used], us_sem, ur_sem
    )
    u_move.start()
    relay(9)
    u_move.wait()
    total = part[rep, :, used]
    for shift in range(1, replicas):
        total = total + recv[lax.rem(rep + shift, replicas), :, used]
    full[rep, :, used] = total / replicas
    ua_move = Exchange(
        "dp", replicas, rep, lambda peer: full.at[rep, :, used], full.at[rep, :, used], uas_sem, uar_sem
    )
    ua_move.start()
    relay(10)
    ua_move.wait()
    for i in range(replicas):
        pmat[pl.ds(i * lines, lines), used] = full[i, :, used]
    q_mean = pmat[:, used]
    q_out[...] = q_mean
    upper, lower = split_parts(q_mean)
    yv[pl.ds(gathered, rank), :] = upper
    yv[pl.ds(gathered + rank, rank), :] = lower
    yv[pl.ds(gathered + 2 * rank, rank), :] = upper

    tall = xt.shape[0]
    wide = 512 if width % 512 == 0 else 256

    def tile(t):
        rows = pl.ds(pl.multiple_of(t * tall, tall), tall)
        xt[...] = xg[:, rows].T

        def column(n, carry):
            cols = pl.ds(pl.multiple_of(n * wide, wide), wide)
            e_ref[rows, cols] = jnp.dot(
                xt[...], yv[:, cols], preferred_element_type=F32
            ).astype(BF16)
            return carry

        lax.fori_loop(0, width // wide, column, 0)

    tiles = depth // tall
    each = tall // chunk
    last = CHUNKS + shards - 1
    start = last - tiles

    def late(step, carry):
        relay(step)
        return carry

    lax.fori_loop(EARLY, max(start, EARLY), late, 0)

    def finish(t, carry):
        tile(t)
        step = t + max(start, EARLY)

        @pl.when(step < last)
        def _():
            relay(step)

        return carry

    safe = min(tiles, max(start, EARLY) and tiles - 1)
    lax.fori_loop(0, safe, finish, 0)
    for step in range(safe + max(start, EARLY), last):
        relay(step)
    for t in range(safe, tiles):
        tile(t)

    def drain(c, carry):
        for h in range(shards - 1):

            @pl.when(jnp.logical_and(me - h >= 0, me < shards - 1))
            def _():
                hop(me - h, c, right_send.at[h, c], right_recv.at[h, c], me + 1).wait_send()

            @pl.when(jnp.logical_and(me + h < shards, me > 0))
            def _():
                hop(me + h, c, left_send.at[h, c], left_recv.at[h, c], me - 1).wait_send()

        return carry

    lax.fori_loop(0, CHUNKS, drain, 0)


def write_kernel(error_ref, q_ref, error_out, q_out, sem):
    parts = sem.shape[0]
    rows = error_ref.shape[0] // parts
    copies = []
    for k in range(parts):
        here = pl.ds(k * rows, rows)
        copies.append(
            pltpu.make_async_copy(error_ref.at[here, :], error_out.at[here, :], sem.at[k])
        )
        copies[-1].start()
    q_out[...] = q_ref[...].T
    for copy in copies:
        copy.wait()


def write_out(error, q_mean):
    depth, width = error.shape
    vmem = pl.BlockSpec(memory_space=pltpu.VMEM)
    return pl.pallas_call(
        write_kernel,
        out_shape=(
            jax.ShapeDtypeStruct((depth, width), error.dtype),
            jax.ShapeDtypeStruct((width, q_mean.shape[0]), q_mean.dtype),
        ),
        in_specs=[vmem, vmem],
        out_specs=(pl.BlockSpec(memory_space=pl.ANY), vmem),
        scratch_shapes=[pltpu.SemaphoreType.DMA((8,))],
        compiler_params=pltpu.CompilerParams(vmem_limit_bytes=8 * 2**20),
        name="write_out",
    )(error, q_mean)


def per_device(activations, output_grads, q_start):
    replicas = lax.axis_size("dp")
    shards = lax.axis_size("mp")
    tokens, depth = activations.shape
    gathered, width = output_grads.shape
    rank = q_start.shape[1]
    lines = rank // replicas
    span = depth // shards
    inner = gathered + 256
    dma = pltpu.SemaphoreType.DMA
    any_space = pl.BlockSpec(memory_space=pl.ANY)
    vmem = pl.BlockSpec(memory_space=pltpu.VMEM)
    error, q_mean = pl.pallas_call(
        functools.partial(step_kernel, (replicas, shards)),
        out_shape=(
            pltpu.VMEM((depth, width), BF16),
            jax.ShapeDtypeStruct((rank, width), F32),
        ),
        in_specs=[any_space, any_space, vmem],
        out_specs=(vmem, vmem),
        scratch_shapes=[
            pltpu.VMEM((inner, depth), BF16),
            pltpu.VMEM((inner, width), BF16),
            pltpu.VMEM((512, inner), BF16),
            pltpu.VMEM((shards, rank, tokens), F32),
            pltpu.VMEM((shards, rank, tokens), F32),
            pltpu.VMEM((replicas, lines, depth), F32),
            pltpu.VMEM((replicas, lines, depth), F32),
            pltpu.VMEM((replicas, lines, depth), F32),
            pltpu.VMEM((rank, depth), F32),
            pltpu.VMEM((shards, lines, span), F32),
            pltpu.VMEM((shards, lines, span), F32),
            pltpu.VMEM((shards, lines, span), F32),
            pltpu.VMEM((shards, rank, tokens), F32),
            dma((2,)),
        ]
        + [dma((shards,))] * 2
        + [dma((replicas,))] * 2
        + [dma((shards,))] * 4
        + [dma((replicas,))] * 2
        + [dma((shards,))] * 2
        + [dma((replicas,))] * 4
        + [dma((shards, CHUNKS))] * 4,
        compiler_params=pltpu.CompilerParams(
            collective_id=0, has_side_effects=True, vmem_limit_bytes=35 * 2**20
        ),
        name="step",
    )(activations, output_grads, q_start)
    return write_out(error, q_mean)


def solution(mesh):
    in_specs = (P(("dp", "mp"), None), P("dp", "mp"), P("mp", None))
    out_specs = (P("dp", "mp"), P("mp", None))
    return jax.shard_map(
        per_device, mesh=mesh, in_specs=in_specs, out_specs=out_specs, check_vma=False
    )
```

```python
import functools

import jax
import jax.numpy as jnp
from jax import lax
from jax.experimental import pallas as pl
from jax.experimental.pallas import tpu as pltpu
from jax.sharding import PartitionSpec as P

ROWS = (((0,), (0,)), ((), ()))
COLS = (((1,), (1,)), ((), ()))
MESH = pl.DeviceIdType.MESH
F32 = jnp.float32
BF16 = jnp.bfloat16
CHUNKS = 16
EARLY = 14
EARLY_TILES = 5


def split_parts(values):
    upper = values.astype(BF16)
    lower = (values - upper.astype(F32)).astype(BF16)
    return (upper, lower)


def inverse_factor(gram):
    rank = gram.shape[0]
    row = lax.broadcasted_iota(jnp.int32, (rank, rank), 0)
    col = lax.broadcasted_iota(jnp.int32, (rank, rank), 1)
    left = gram
    right = jnp.where(row == col, 1.0, 0.0).astype(F32)
    down = lax.broadcasted_iota(jnp.int32, (rank, 1), 0)
    pivots = jnp.ones((rank, 1), F32)
    for k in range(rank):
        pivot = left[k : k + 1, k : k + 1]
        pivots = jnp.where(down == k, pivot, pivots)
        factor = jnp.where(down > k, left[:, k : k + 1] / pivot, 0.0)
        left_row = left[k : k + 1, :]
        right_row = right[k : k + 1, :]
        left = left - factor * left_row
        right = right - factor * right_row
    return right / jnp.sqrt(pivots)


class Exchange:
    def __init__(self, axis, count, me, source, target, send_sem, recv_sem):
        self.copies = []
        for shift in range(1, count):
            peer = lax.rem(me + shift, count)
            self.copies.append(
                pltpu.make_async_remote_copy(
                    src_ref=source(peer),
                    dst_ref=target,
                    send_sem=send_sem.at[shift],
                    recv_sem=recv_sem.at[shift],
                    device_id={axis: peer},
                    device_id_type=MESH,
                )
            )

    def start(self):
        for copy in self.copies:
            copy.start()

    def wait(self):
        for copy in self.copies:
            copy.wait()


def step_kernel(
    dims,
    x_hbm,
    y_hbm,
    q_ref,
    e_ref,
    q_out,
    xg,
    yv,
    xown,
    pcat,
    zpart,
    zrecv,
    part,
    recv,
    full,
    pmat,
    psum,
    pzr,
    pz,
    wall,
    upart,
    urecv,
    ufull,
    local_sem,
    zs_sem,
    zr_sem,
    ps_sem,
    pr_sem,
    pzs_sem,
    pzr_sem,
    ags_sem,
    agr_sem,
    pgs_sem,
    pgr_sem,
    ws_sem,
    wr_sem,
    us_sem,
    ur_sem,
    uas_sem,
    uar_sem,
    right_send,
    right_recv,
    left_send,
    left_recv,
):
    replicas, shards = dims
    me = lax.axis_index("mp")
    rep = lax.axis_index("dp")
    tokens, depth = x_hbm.shape
    gathered, width = y_hbm.shape
    rank = q_ref.shape[0]
    lines = rank // replicas
    span = depth // shards
    chunk = depth // CHUNKS
    highest = lax.Precision.HIGHEST

    x_copy = pltpu.make_async_copy(x_hbm, xown, local_sem.at[0])
    y_copy = pltpu.make_async_copy(y_hbm, yv.at[pl.ds(0, gathered), :], local_sem.at[1])
    x_copy.start()
    y_copy.start()

    barrier = pltpu.get_barrier_semaphore()
    for shift in range(1, shards):
        peer = lax.rem(me + shift, shards)
        pl.semaphore_signal(barrier, inc=1, device_id={"mp": peer}, device_id_type=MESH)
    for shift in range(1, replicas):
        peer = lax.rem(rep + shift, replicas)
        pl.semaphore_signal(barrier, inc=1, device_id={"dp": peer}, device_id_type=MESH)
    pl.semaphore_wait(barrier, shards + replicas - 2)

    def hop(owner, c, send_sem, recv_sem, target):
        block = xg.at[owner, pl.ds(pl.multiple_of(c * chunk, chunk), chunk), :]
        return pltpu.make_async_remote_copy(
            src_ref=block,
            dst_ref=block,
            send_sem=send_sem,
            recv_sem=recv_sem,
            device_id={"mp": target},
            device_id_type=MESH,
        )

    def turn(c):
        if c < CHUNKS:
            cols = pl.ds(c * chunk, chunk)
            xg[me, cols, :] = xown[:, cols].T

    def relay(step):
        turn(step + 1)
        for h in range(shards):
            c = step - h
            inside = jnp.logical_and(c >= 0, c < CHUNKS)
            for ahead, sends, recvs in ((True, right_send, right_recv), (False, left_send, left_recv)):
                owner = me - h if ahead else me + h
                exists = owner >= 0 if ahead else owner < shards
                onward = me < shards - 1 if ahead else me > 0
                target = me + 1 if ahead else me - 1
                source = me - 1 if ahead else me + 1
                if h >= 1:

                    @pl.when(jnp.logical_and(inside, exists))
                    def _():
                        hop(owner, c, sends.at[h - 1, c], recvs.at[h - 1, c], source).wait_recv()

                if h < shards - 1:

                    @pl.when(jnp.logical_and(inside, jnp.logical_and(exists, onward)))
                    def _():
                        hop(owner, c, sends.at[h, c], recvs.at[h, c], target).start()

    tall = 2 * chunk
    wide = width // 2
    blocks = range(shards)

    def sweep(body):
        def column(n, carry):
            body(pl.ds(pl.multiple_of(n * wide, wide), wide))
            return carry

        lax.fori_loop(0, width // wide, column, 0)

    def draft(first, size):
        rows = pl.ds(first, size)

        def body(cols):
            lhs = jnp.concatenate([xg[b, rows, :] for b in blocks], axis=1)
            e_ref[rows, cols] = jnp.dot(
                lhs, yv[pl.ds(0, gathered), cols], preferred_element_type=F32
            ).astype(BF16)

        sweep(body)

    def patch(first, size):
        rows = pl.ds(first, size)

        def body(cols):
            low = jnp.dot(
                pcat[rows, :], yv[pl.ds(gathered, inner), cols], preferred_element_type=F32
            )
            e_ref[rows, cols] = (e_ref[rows, cols].astype(F32) + low).astype(BF16)

        sweep(body)

    def tile(first, size):
        rows = pl.ds(first, size)

        def body(cols):
            lhs = jnp.concatenate([xg[b, rows, :] for b in blocks] + [pcat[rows, :]], axis=1)
            e_ref[rows, cols] = jnp.dot(lhs, yv[:, cols], preferred_element_type=F32).astype(BF16)

        sweep(body)

    x_copy.wait()
    turn(0)
    relay(0)

    q_cat = jnp.concatenate(split_parts(q_ref[...]), axis=0)
    inner = yv.shape[0] - gathered
    yv[pl.ds(gathered + 2 * rank, inner - 2 * rank), :] = jnp.zeros((inner - 2 * rank, width), BF16)
    y_copy.wait()
    both = lax.dot_general(yv[pl.ds(0, gathered), :], q_cat, COLS, preferred_element_type=F32)
    both = both.T
    projected = both[:rank] + both[rank:]
    for j in range(shards):
        zpart[j] = projected[:, j * tokens : (j + 1) * tokens].astype(zpart.dtype)
    z_move = Exchange("mp", shards, me, lambda peer: zpart.at[peer], zrecv.at[me], zs_sem, zr_sem)
    z_move.start()
    relay(1)
    z_move.wait()
    total = zpart[me].astype(F32)
    for shift in range(1, shards):
        total = total + zrecv[lax.rem(me + shift, shards)].astype(F32)

    z_cat = jnp.concatenate(split_parts(total), axis=0)
    both = jnp.dot(z_cat, xown[...], preferred_element_type=F32)
    left = both[:rank] + both[rank:]
    for i in range(replicas):
        part[i] = left[i * lines : (i + 1) * lines, :]
    p_move = Exchange("dp", replicas, rep, lambda peer: part.at[peer], recv.at[rep], ps_sem, pr_sem)
    p_move.start()
    relay(2)
    relay(3)
    p_move.wait()
    total = part[rep]
    for shift in range(1, replicas):
        total = total + recv[lax.rem(rep + shift, replicas)]
    for j in range(shards):
        psum[j] = total[:, j * span : (j + 1) * span]
    pz_move = Exchange("mp", shards, me, lambda peer: psum.at[peer], pzr.at[me], pzs_sem, pzr_sem)
    pz_move.start()
    relay(4)
    pz_move.wait()
    total = psum[me]
    for shift in range(1, shards):
        total = total + pzr[lax.rem(me + shift, shards)]
    pz[me] = total / replicas
    ag_move = Exchange("mp", shards, me, lambda peer: pz.at[me], pz.at[me], ags_sem, agr_sem)
    ag_move.start()
    relay(5)
    ag_move.wait()
    for j in range(shards):
        full[rep, :, pl.ds(j * span, span)] = pz[j]
    pg_move = Exchange("dp", replicas, rep, lambda peer: full.at[rep], full.at[rep], pgs_sem, pgr_sem)
    pg_move.start()
    relay(6)
    draft(0, tall)
    relay(7)
    pg_move.wait()
    for i in range(replicas):
        pmat[pl.ds(i * lines, lines), :] = full[i]
    relay(8)
    draft(tall, tall)

    p_mean = pmat[...]
    gram = lax.dot_general(p_mean, p_mean, COLS, precision=highest, preferred_element_type=F32)
    inverse = inverse_factor(gram)
    ortho = jnp.dot(inverse, pmat[...], precision=highest, preferred_element_type=F32)
    ortho_cat = jnp.concatenate(split_parts(-ortho), axis=0)

    both = lax.dot_general(ortho_cat, xown[...], COLS, preferred_element_type=F32)
    wall[me] = -(both[:rank] + both[rank:]).astype(wall.dtype)
    w_move = Exchange("mp", shards, me, lambda peer: wall.at[me], wall.at[me], ws_sem, wr_sem)
    w_move.start()
    pcat[:, pl.ds(0, 2 * rank)] = ortho_cat.T
    pcat[:, pl.ds(2 * rank, inner - 2 * rank)] = jnp.zeros((depth, inner - 2 * rank), BF16)
    relay(9)
    w_move.wait()
    seen = jnp.concatenate([wall[j] for j in range(shards)], axis=1)
    right = jnp.dot(seen, yv[pl.ds(0, gathered), :], preferred_element_type=F32)
    used = pl.ds(0, width)
    for i in range(replicas):
        upart[i] = right[i * lines : (i + 1) * lines, :].astype(BF16)
    u_move = Exchange("dp", replicas, rep, lambda peer: upart.at[peer], urecv.at[rep], us_sem, ur_sem)
    u_move.start()
    relay(10)
    draft(2 * tall, tall)
    relay(11)
    u_move.wait()
    total = upart[rep].astype(F32)
    for shift in range(1, replicas):
        total = total + urecv[lax.rem(rep + shift, replicas)].astype(F32)
    ufull[rep] = (total / replicas).astype(BF16)
    ua_move = Exchange("dp", replicas, rep, lambda peer: ufull.at[rep], ufull.at[rep], uas_sem, uar_sem)
    ua_move.start()
    relay(12)
    draft(3 * tall, tall)
    relay(13)
    draft(4 * tall, tall)
    ua_move.wait()
    for i in range(replicas):
        pmat[pl.ds(i * lines, lines), used] = ufull[i].astype(F32)
    q_mean = pmat[:, used]
    q_out[...] = q_mean
    upper = q_mean.astype(BF16)
    yv[pl.ds(gathered, rank), :] = upper
    yv[pl.ds(gathered + rank, rank), :] = upper

    for t in range(EARLY_TILES):
        patch(t * tall, tall)
    halves = CHUNKS // 2
    last = CHUNKS + shards - 1
    done = EARLY
    for t in range(EARLY_TILES, halves - 1):
        for step in range(done, 2 * t + shards + 1):
            relay(step)
        done = max(done, 2 * t + shards + 1)
        tile(t * tall, tall)
    for t in (CHUNKS - 2, CHUNKS - 1):
        for step in range(done, t + shards):
            relay(step)
        done = max(done, t + shards)
        tile(t * chunk, chunk)

    def drain(c, carry):
        for h in range(shards - 1):

            @pl.when(jnp.logical_and(me - h >= 0, me < shards - 1))
            def _():
                hop(me - h, c, right_send.at[h, c], right_recv.at[h, c], me + 1).wait_send()

            @pl.when(jnp.logical_and(me + h < shards, me > 0))
            def _():
                hop(me + h, c, left_send.at[h, c], left_recv.at[h, c], me - 1).wait_send()

        return carry

    lax.fori_loop(0, CHUNKS, drain, 0)


def write_kernel(error_ref, q_ref, error_out, q_out, sem):
    parts = sem.shape[0] - 1
    rows = error_ref.shape[0] // parts
    copies = []
    for k in range(parts):
        here = pl.ds(k * rows, rows)
        copies.append(
            pltpu.make_async_copy(error_ref.at[here, :], error_out.at[here, :], sem.at[k])
        )
        copies[-1].start()
    q_copy = pltpu.make_async_copy(q_ref, q_out, sem.at[parts])
    q_copy.start()
    for copy in copies:
        copy.wait()
    q_copy.wait()


def write_out(error, q_mean):
    vmem = pl.BlockSpec(memory_space=pltpu.VMEM)
    hbm = pl.BlockSpec(memory_space=pl.ANY)
    return pl.pallas_call(
        write_kernel,
        out_shape=(
            jax.ShapeDtypeStruct(error.shape, error.dtype),
            jax.ShapeDtypeStruct(q_mean.shape, q_mean.dtype),
        ),
        in_specs=[vmem, vmem],
        out_specs=(hbm, hbm),
        scratch_shapes=[pltpu.SemaphoreType.DMA((9,))],
        compiler_params=pltpu.CompilerParams(vmem_limit_bytes=2 * 2**20),
        name="write_out",
    )(error, q_mean)


def per_device(activations, output_grads, q_start):
    replicas = lax.axis_size("dp")
    shards = lax.axis_size("mp")
    tokens, depth = activations.shape
    gathered, width = output_grads.shape
    rank = q_start.shape[1]
    lines = rank // replicas
    span = depth // shards
    inner = 256
    dma = pltpu.SemaphoreType.DMA
    any_space = pl.BlockSpec(memory_space=pl.ANY)
    vmem = pl.BlockSpec(memory_space=pltpu.VMEM)
    error, q_mean = pl.pallas_call(
        functools.partial(step_kernel, (replicas, shards)),
        out_shape=(
            pltpu.VMEM((depth, width), BF16),
            pltpu.VMEM((rank, width), F32),
        ),
        in_specs=[any_space, any_space, vmem],
        out_specs=(vmem, vmem),
        scratch_shapes=[
            pltpu.VMEM((shards, depth, tokens), BF16),
            pltpu.VMEM((gathered + inner, width), BF16),
            pltpu.VMEM((tokens, depth), BF16),
            pltpu.VMEM((depth, inner), BF16),
            pltpu.VMEM((shards, rank, tokens), BF16),
            pltpu.VMEM((shards, rank, tokens), BF16),
            pltpu.VMEM((replicas, lines, depth), F32),
            pltpu.VMEM((replicas, lines, depth), F32),
            pltpu.VMEM((replicas, lines, depth), F32),
            pltpu.VMEM((rank, depth), F32),
            pltpu.VMEM((shards, lines, span), F32),
            pltpu.VMEM((shards, lines, span), F32),
            pltpu.VMEM((shards, lines, span), F32),
            pltpu.VMEM((shards, rank, tokens), BF16),
            pltpu.VMEM((replicas, lines, width), BF16),
            pltpu.VMEM((replicas, lines, width), BF16),
            pltpu.VMEM((replicas, lines, width), BF16),
            dma((2,)),
        ]
        + [dma((shards,))] * 2
        + [dma((replicas,))] * 2
        + [dma((shards,))] * 4
        + [dma((replicas,))] * 2
        + [dma((shards,))] * 2
        + [dma((replicas,))] * 4
        + [dma((shards, CHUNKS))] * 4,
        compiler_params=pltpu.CompilerParams(
            collective_id=0, has_side_effects=True, vmem_limit_bytes=34 * 2**20
        ),
        name="step",
    )(activations, output_grads, q_start.T)
    error, q_mean = write_out(error, q_mean)
    return (error, q_mean.T)


def solution(mesh):
    in_specs = (P(("dp", "mp"), None), P("dp", "mp"), P("mp", None))
    out_specs = (P("dp", "mp"), P("mp", None))
    return jax.shard_map(
        per_device, mesh=mesh, in_specs=in_specs, out_specs=out_specs, check_vma=False
    )
```

```python
import functools

import jax
import jax.numpy as jnp
from jax import lax
from jax.experimental import pallas as pl
from jax.experimental.pallas import tpu as pltpu
from jax.sharding import PartitionSpec as P

ROWS = (((0,), (0,)), ((), ()))
COLS = (((1,), (1,)), ((), ()))
MESH = pl.DeviceIdType.MESH
F32 = jnp.float32
BF16 = jnp.bfloat16
CHUNKS = 16


def split_parts(values):
    upper = values.astype(BF16)
    lower = (values - upper.astype(F32)).astype(BF16)
    return (upper, lower)


def inverse_factor(gram, between):
    rank = gram.shape[0]
    row = lax.broadcasted_iota(jnp.int32, (rank, rank), 0)
    col = lax.broadcasted_iota(jnp.int32, (rank, rank), 1)
    left = gram
    right = jnp.where(row == col, 1.0, 0.0).astype(F32)
    down = lax.broadcasted_iota(jnp.int32, (rank, 1), 0)
    pivots = jnp.ones((rank, 1), F32)
    for k in range(rank):
        pivot = left[k : k + 1, k : k + 1]
        pivots = jnp.where(down == k, pivot, pivots)
        if k == rank // 2:
            between()
        factor = jnp.where(down > k, left[:, k : k + 1] / pivot, 0.0)
        left_row = left[k : k + 1, :]
        right_row = right[k : k + 1, :]
        left = left - factor * left_row
        right = right - factor * right_row
    return right / jnp.sqrt(pivots)


class Exchange:
    def __init__(self, axis, count, me, source, target, send_sem, recv_sem):
        self.copies = []
        for shift in range(1, count):
            peer = lax.rem(me + shift, count)
            self.copies.append(
                pltpu.make_async_remote_copy(
                    src_ref=source(peer),
                    dst_ref=target,
                    send_sem=send_sem.at[shift],
                    recv_sem=recv_sem.at[shift],
                    device_id={axis: peer},
                    device_id_type=MESH,
                )
            )

    def start(self):
        for copy in self.copies:
            copy.start()

    def wait(self):
        for copy in self.copies:
            copy.wait()


def step_kernel(
    dims,
    x_hbm,
    y_hbm,
    q_ref,
    e_ref,
    q_out,
    xg,
    yv,
    xown,
    pcat,
    zpart,
    zrecv,
    part,
    recv,
    full,
    pmat,
    psum,
    pzr,
    pz,
    wall,
    upart,
    urecv,
    ufull,
    local_sem,
    zs_sem,
    zr_sem,
    ps_sem,
    pr_sem,
    pzs_sem,
    pzr_sem,
    ags_sem,
    agr_sem,
    pgs_sem,
    pgr_sem,
    ws_sem,
    wr_sem,
    us_sem,
    ur_sem,
    uas_sem,
    uar_sem,
    right_send,
    right_recv,
    left_send,
    left_recv,
):
    replicas, shards = dims
    me = lax.axis_index("mp")
    rep = lax.axis_index("dp")
    tokens, depth = x_hbm.shape
    gathered, width = y_hbm.shape
    rank = q_ref.shape[0]
    lines = rank // replicas
    span = depth // shards
    chunk = depth // CHUNKS
    tall = 2 * chunk
    highest = lax.Precision.HIGHEST

    x_copy = pltpu.make_async_copy(x_hbm, xown, local_sem.at[0])
    y_copy = pltpu.make_async_copy(y_hbm, yv.at[pl.ds(0, gathered), :], local_sem.at[1])
    x_copy.start()
    y_copy.start()

    barrier = pltpu.get_barrier_semaphore()
    for shift in range(1, shards):
        peer = lax.rem(me + shift, shards)
        pl.semaphore_signal(barrier, inc=1, device_id={"mp": peer}, device_id_type=MESH)
    for shift in range(1, replicas):
        peer = lax.rem(rep + shift, replicas)
        pl.semaphore_signal(barrier, inc=1, device_id={"dp": peer}, device_id_type=MESH)
    pl.semaphore_wait(barrier, shards + replicas - 2)

    def hop(owner, c, send_sem, recv_sem, target):
        block = xg.at[owner, pl.ds(pl.multiple_of(c * chunk, chunk), chunk), :]
        return pltpu.make_async_remote_copy(
            src_ref=block,
            dst_ref=block,
            send_sem=send_sem,
            recv_sem=recv_sem,
            device_id={"mp": target},
            device_id_type=MESH,
        )

    def turn(c):
        if c < CHUNKS:
            cols = pl.ds(c * chunk, chunk)
            xg[me, cols, :] = xown[:, cols].T

    def relay(step):
        turn(step + 2)
        for h in range(shards - 1):
            c = step + 1 if h == 0 else step - h
            if c < 0 or c >= CHUNKS:
                continue
            for ahead, sends, recvs in ((True, right_send, right_recv), (False, left_send, left_recv)):
                owner = me - h if ahead else me + h
                exists = owner >= 0 if ahead else owner < shards
                onward = me < shards - 1 if ahead else me > 0
                target = me + 1 if ahead else me - 1
                source = me - 1 if ahead else me + 1

                @pl.when(jnp.logical_and(exists, onward))
                def _():
                    if h >= 1:
                        hop(owner, c, sends.at[h - 1, c], recvs.at[h - 1, c], source).wait_recv()
                    hop(owner, c, sends.at[h, c], recvs.at[h, c], target).start()

    def arrive(c):
        @pl.when(me == shards - 1)
        def _():
            for h in range(1, shards):
                hop(me - h, c, right_send.at[h - 1, c], right_recv.at[h - 1, c], me - 1).wait_recv()

        @pl.when(me == 0)
        def _():
            for h in range(1, shards):
                hop(me + h, c, left_send.at[h - 1, c], left_recv.at[h - 1, c], me + 1).wait_recv()

    state = {"relay": -1, "draft": 0}
    halves = CHUNKS // 2
    last = CHUNKS + shards - 2

    def advance(count):
        for _ in range(count):
            if state["relay"] < last:
                relay(state["relay"])
                state["relay"] += 1

    def early(count):
        for _ in range(count):
            t = state["draft"]
            if t < halves - 1 and 2 * t + shards < state["relay"]:
                arrive(2 * t)
                arrive(2 * t + 1)
                draft(t * tall, tall)
                state["draft"] += 1

    wide = width // 2
    blocks = range(shards)

    def sweep(body):
        def column(n, carry):
            body(pl.ds(pl.multiple_of(n * wide, wide), wide))
            return carry

        lax.fori_loop(0, width // wide, column, 0)

    def draft(first, size):
        rows = pl.ds(first, size)

        def body(cols):
            lhs = jnp.concatenate([xg[b, rows, :] for b in blocks], axis=1)
            e_ref[rows, cols] = jnp.dot(
                lhs, yv[pl.ds(0, gathered), cols], preferred_element_type=F32
            ).astype(BF16)

        sweep(body)

    def patch(first, size):
        rows = pl.ds(first, size)

        def body(cols):
            low = jnp.dot(
                pcat[rows, :], yv[pl.ds(gathered, inner), cols], preferred_element_type=F32
            )
            e_ref[rows, cols] = (e_ref[rows, cols].astype(F32) + low).astype(BF16)

        sweep(body)

    def tile(first, size):
        rows = pl.ds(first, size)

        def body(cols):
            lhs = jnp.concatenate([xg[b, rows, :] for b in blocks] + [pcat[rows, :]], axis=1)
            e_ref[rows, cols] = jnp.dot(lhs, yv[:, cols], preferred_element_type=F32).astype(BF16)

        sweep(body)

    x_copy.wait()
    turn(0)
    turn(1)
    advance(2)

    q_cat = jnp.concatenate(split_parts(q_ref[...]), axis=0)
    inner = yv.shape[0] - gathered
    yv[pl.ds(gathered + 3 * rank, inner - 3 * rank), :] = jnp.zeros((inner - 3 * rank, width), BF16)
    y_copy.wait()
    both = lax.dot_general(yv[pl.ds(0, gathered), :], q_cat, COLS, preferred_element_type=F32)
    both = both.T
    projected = both[:rank] + both[rank:]
    for j in range(shards):
        zpart[j] = projected[:, j * tokens : (j + 1) * tokens].astype(zpart.dtype)
    z_move = Exchange("mp", shards, me, lambda peer: zpart.at[peer], zrecv.at[me], zs_sem, zr_sem)
    z_move.start()
    advance(1)
    z_move.wait()
    total = zpart[me].astype(F32)
    for shift in range(1, shards):
        total = total + zrecv[lax.rem(me + shift, shards)].astype(F32)

    z_cat = jnp.concatenate(split_parts(total), axis=0)
    both = jnp.dot(z_cat, xown[...], preferred_element_type=F32)
    left = both[:rank] + both[rank:]
    for i in range(replicas):
        part[i] = left[i * lines : (i + 1) * lines, :]
    p_move = Exchange("dp", replicas, rep, lambda peer: part.at[peer], recv.at[rep], ps_sem, pr_sem)
    p_move.start()
    advance(2)
    p_move.wait()
    total = part[rep]
    for shift in range(1, replicas):
        total = total + recv[lax.rem(rep + shift, replicas)]
    for j in range(shards):
        psum[j] = total[:, j * span : (j + 1) * span].astype(BF16)
    pz_move = Exchange("mp", shards, me, lambda peer: psum.at[peer], pzr.at[me], pzs_sem, pzr_sem)
    pz_move.start()
    advance(1)
    pz_move.wait()
    total = psum[me].astype(F32)
    for shift in range(1, shards):
        total = total + pzr[lax.rem(me + shift, shards)].astype(F32)
    pz[me] = (total / replicas).astype(BF16)
    ag_move = Exchange("mp", shards, me, lambda peer: pz.at[me], pz.at[me], ags_sem, agr_sem)
    ag_move.start()
    advance(1)
    ag_move.wait()
    for j in range(shards):
        full[rep, :, pl.ds(j * span, span)] = pz[j].astype(F32)
    pg_move = Exchange("dp", replicas, rep, lambda peer: full.at[rep], full.at[rep], pgs_sem, pgr_sem)
    pg_move.start()
    advance(1)
    early(1)
    advance(1)
    pg_move.wait()
    for i in range(replicas):
        pmat[pl.ds(i * lines, lines), :] = full[i]
    advance(1)

    p_mean = pmat[...]
    gram = lax.dot_general(p_mean, p_mean, COLS, precision=highest, preferred_element_type=F32)
    inverse = inverse_factor(gram, lambda: advance(1))
    ortho = jnp.dot(inverse, pmat[...], precision=highest, preferred_element_type=F32)
    ortho_cat = jnp.concatenate(split_parts(-ortho), axis=0)

    both = lax.dot_general(ortho_cat, xown[...], COLS, preferred_element_type=F32)
    wall[me] = -(both[:rank] + both[rank:]).astype(wall.dtype)
    w_move = Exchange("mp", shards, me, lambda peer: wall.at[me], wall.at[me], ws_sem, wr_sem)
    w_move.start()
    turned = ortho_cat.T
    pcat[:, pl.ds(0, 2 * rank)] = turned
    pcat[:, pl.ds(2 * rank, rank)] = turned[:, :rank]
    pcat[:, pl.ds(3 * rank, inner - 3 * rank)] = jnp.zeros((depth, inner - 3 * rank), BF16)
    early(1)
    advance(1)
    w_move.wait()
    seen = jnp.concatenate([wall[j] for j in range(shards)], axis=1)
    right = jnp.dot(seen, yv[pl.ds(0, gathered), :], preferred_element_type=F32)
    used = pl.ds(0, width)
    for i in range(replicas):
        upart[i] = right[i * lines : (i + 1) * lines, :]
    u_move = Exchange("dp", replicas, rep, lambda peer: upart.at[peer], urecv.at[rep], us_sem, ur_sem)
    u_move.start()
    advance(1)
    early(1)
    advance(1)
    u_move.wait()
    total = upart[rep]
    for shift in range(1, replicas):
        total = total + urecv[lax.rem(rep + shift, replicas)]
    ufull[rep] = total / replicas
    ua_move = Exchange("dp", replicas, rep, lambda peer: ufull.at[rep], ufull.at[rep], uas_sem, uar_sem)
    ua_move.start()
    advance(1)
    early(1)
    advance(1)
    early(1)
    ua_move.wait()
    for i in range(replicas):
        pmat[pl.ds(i * lines, lines), used] = ufull[i]
    q_mean = pmat[:, used]
    q_out[...] = q_mean
    upper, lower = split_parts(q_mean)
    yv[pl.ds(gathered, rank), :] = upper
    yv[pl.ds(gathered + rank, rank), :] = upper
    yv[pl.ds(gathered + 2 * rank, rank), :] = lower
    advance(1)
    for t in range(state["draft"]):
        patch(t * tall, tall)
        advance(1)
    advance(last)
    for t in range(state["draft"], halves - 1):
        arrive(2 * t)
        arrive(2 * t + 1)
        tile(t * tall, tall)
    for t in (CHUNKS - 2, CHUNKS - 1):
        arrive(t)
        tile(t * chunk, chunk)

    def drain(c, carry):
        for h in range(shards - 1):

            @pl.when(jnp.logical_and(me - h >= 0, me < shards - 1))
            def _():
                hop(me - h, c, right_send.at[h, c], right_recv.at[h, c], me + 1).wait_send()

            @pl.when(jnp.logical_and(me + h < shards, me > 0))
            def _():
                hop(me + h, c, left_send.at[h, c], left_recv.at[h, c], me - 1).wait_send()

        return carry

    lax.fori_loop(0, CHUNKS, drain, 0)


def write_kernel(error_ref, q_ref, error_out, q_out, sem):
    parts = sem.shape[0] - 1
    rows = error_ref.shape[0] // parts
    copies = []
    for k in range(parts):
        here = pl.ds(k * rows, rows)
        copies.append(
            pltpu.make_async_copy(error_ref.at[here, :], error_out.at[here, :], sem.at[k])
        )
        copies[-1].start()
    q_copy = pltpu.make_async_copy(q_ref, q_out, sem.at[parts])
    q_copy.start()
    for copy in copies:
        copy.wait()
    q_copy.wait()


def write_out(error, q_mean):
    vmem = pl.BlockSpec(memory_space=pltpu.VMEM)
    hbm = pl.BlockSpec(memory_space=pl.ANY)
    return pl.pallas_call(
        write_kernel,
        out_shape=(
            jax.ShapeDtypeStruct(error.shape, error.dtype),
            jax.ShapeDtypeStruct(q_mean.shape, q_mean.dtype),
        ),
        in_specs=[vmem, vmem],
        out_specs=(hbm, hbm),
        scratch_shapes=[pltpu.SemaphoreType.DMA((9,))],
        compiler_params=pltpu.CompilerParams(vmem_limit_bytes=2 * 2**20),
        name="write_out",
    )(error, q_mean)


def per_device(activations, output_grads, q_start):
    replicas = lax.axis_size("dp")
    shards = lax.axis_size("mp")
    tokens, depth = activations.shape
    gathered, width = output_grads.shape
    rank = q_start.shape[1]
    lines = rank // replicas
    span = depth // shards
    inner = 256
    dma = pltpu.SemaphoreType.DMA
    any_space = pl.BlockSpec(memory_space=pl.ANY)
    vmem = pl.BlockSpec(memory_space=pltpu.VMEM)
    error, q_mean = pl.pallas_call(
        functools.partial(step_kernel, (replicas, shards)),
        out_shape=(
            pltpu.VMEM((depth, width), BF16),
            pltpu.VMEM((rank, width), F32),
        ),
        in_specs=[any_space, any_space, vmem],
        out_specs=(vmem, vmem),
        scratch_shapes=[
            pltpu.VMEM((shards, depth, tokens), BF16),
            pltpu.VMEM((gathered + inner, width), BF16),
            pltpu.VMEM((tokens, depth), BF16),
            pltpu.VMEM((depth, inner), BF16),
            pltpu.VMEM((shards, rank, tokens), BF16),
            pltpu.VMEM((shards, rank, tokens), BF16),
            pltpu.VMEM((replicas, lines, depth), F32),
            pltpu.VMEM((replicas, lines, depth), F32),
            pltpu.VMEM((replicas, lines, depth), F32),
            pltpu.VMEM((rank, depth), F32),
            pltpu.VMEM((shards, lines, span), BF16),
            pltpu.VMEM((shards, lines, span), BF16),
            pltpu.VMEM((shards, lines, span), BF16),
            pltpu.VMEM((shards, rank, tokens), BF16),
            pltpu.VMEM((replicas, lines, width), F32),
            pltpu.VMEM((replicas, lines, width), F32),
            pltpu.VMEM((replicas, lines, width), F32),
            dma((2,)),
        ]
        + [dma((shards,))] * 2
        + [dma((replicas,))] * 2
        + [dma((shards,))] * 4
        + [dma((replicas,))] * 2
        + [dma((shards,))] * 2
        + [dma((replicas,))] * 4
        + [dma((shards, CHUNKS))] * 4,
        compiler_params=pltpu.CompilerParams(
            collective_id=0, has_side_effects=True, vmem_limit_bytes=34 * 2**20
        ),
        name="step",
    )(activations, output_grads, q_start.T)
    error, q_mean = write_out(error, q_mean)
    return (error, q_mean.T)


def solution(mesh):
    in_specs = (P(("dp", "mp"), None), P("dp", "mp"), P("mp", None))
    out_specs = (P("dp", "mp"), P("mp", None))
    return jax.shard_map(
        per_device, mesh=mesh, in_specs=in_specs, out_specs=out_specs, check_vma=False
    )
```
